16 devices in a mesh: tp: 2 (over z), ep: 8 (over y, x, core).
Axes of the slice: x: 2, y: 2, z: 2, core: 2. Of those that a mesh axis runs over, the one named last changes fastest.
Arguments:
- x_in: bfloat16 [48, 512, 2048], P('ep', 'tp')
- topk_idx: int32 [48, 512, 6], P('ep', 'tp')
- top_gate: float32 [48, 512, 6], P('ep', 'tp')
- g_attn: bfloat16 [2048], replicated
- w_q: bfloat16 [2048, 3072], P(None, 'tp')
- w_dkv: bfloat16 [2048, 576], replicated
- g_kv: bfloat16 [512], replicated
- w_ukv: bfloat16 [512, 4096], P(None, 'tp')
- w_o: bfloat16 [2048, 2048], P('tp')
- g_ffn: bfloat16 [2048], replicated
- w_gate: bfloat16 [64, 2048, 1408], P(('tp', 'ep'))
- w_up: bfloat16 [64, 2048, 1408], P(('tp', 'ep'))
- w_down: bfloat16 [64, 1408, 2048], P(('tp', 'ep'))
- ws_gate: bfloat16 [2048, 2816], replicated
- ws_up: bfloat16 [2048, 2816], replicated
- ws_down: bfloat16 [2816, 2048], replicated
Outputs:
- output 1: bfloat16 [48, 512, 2048], P('ep', 'tp')
- output 2: bfloat16 [48, 512, 576], P('ep', 'tp')
All inputs are finite; a program needn't handle non-finite values.
Results may differ from the reference program's by a relative error of at most 0.0134779.
Values are sent between devices in bfloat16 or wider.
A program may use at most 1 GiB of HBM per device.

```python
import numpy as np
import jax
import jax.numpy as jnp
from jax import lax

D = 2048
HEADS = 16
KV_RANK = 512
NOPE = 128
ROPE = 64
VDIM = 128
EXPERTS = 64
FF = 1408
SHARED = 2
TOP = 6
BATCH_DEV = 6
SEQ_DEV = 256
TP = 2
EP = 8

BATCH = BATCH_DEV * EP
SEQ = SEQ_DEV * TP
TOK_DEV = BATCH_DEV * SEQ_DEV
MEAN_LOAD = TOK_DEV * TOP // EXPERTS
CAP_DEV = 3 * MEAN_LOAD


def rms_norm(values, gain_vec):
    values32 = values.astype(jnp.float32)
    inv_rms = lax.rsqrt(jnp.mean(values32 * values32, axis=-1, keepdims=True) + 1e-6)
    return (values32 * inv_rms * gain_vec.astype(jnp.float32)).astype(jnp.bfloat16)


def rope_tables(positions, rope_dim):
    half_dim = rope_dim // 2
    inv_freq = 10000.0 ** (-2.0 * jnp.arange(half_dim, dtype=jnp.float32) / rope_dim)
    angles = positions.astype(jnp.float32)[:, None] * inv_freq[None, :]
    return jnp.cos(angles), jnp.sin(angles)


def rotate(values, cos_tab, sin_tab):
    half_dim = values.shape[-1] // 2
    first = values[..., :half_dim].astype(jnp.float32)
    second = values[..., half_dim:].astype(jnp.float32)
    return jnp.concatenate([first * cos_tab - second * sin_tab, second * cos_tab + first * sin_tab], axis=-1).astype(jnp.bfloat16)


def draw_routing(root_key):
    cold_load = MEAN_LOAD // 3
    pattern = np.array([CAP_DEV, cold_load, cold_load, MEAN_LOAD - 2 * cold_load] * (EXPERTS // 4))
    slot_pattern = np.repeat(np.arange(EXPERTS), pattern)
    perm_key, row_key = jax.random.split(root_key)
    expert_perm = jax.random.permutation(perm_key, EXPERTS).astype(jnp.int32)
    grid = expert_perm[slot_pattern].reshape(TOP, TOK_DEV).T
    row_keys = jax.random.split(row_key, TP * EP)
    blocks = jax.vmap(lambda one_key: jax.random.permutation(one_key, grid, axis=0))(row_keys)
    blocks = blocks.reshape(EP, TP, BATCH_DEV, SEQ_DEV, TOP).transpose(0, 2, 1, 3, 4)
    return blocks.reshape(BATCH, SEQ, TOP)


def setup_inputs(seed: int = 0) -> dict:
    root_key = jax.random.key(seed)
    sub_keys = jax.random.split(root_key, 16)

    def draw_normal(which, shape, scale):
        return (jax.random.normal(sub_keys[which], shape, jnp.float32) * scale).astype(jnp.bfloat16)

    def draw_gain(which, gain_len):
        return jax.random.uniform(sub_keys[which], (gain_len,), jnp.float32, 0.5, 1.5).astype(jnp.bfloat16)

    gate_logits = jax.random.normal(sub_keys[2], (BATCH, SEQ, TOP), jnp.float32)
    return {
        'x_in': draw_normal(0, (BATCH, SEQ, D), 1.0),
        'topk_idx': draw_routing(sub_keys[1]),
        'top_gate': jax.nn.softmax(gate_logits, axis=-1),
        'g_attn': draw_gain(3, D),
        'w_q': draw_normal(4, (D, HEADS * (NOPE + ROPE)), 1.5 * D ** -0.5),
        'w_dkv': draw_normal(5, (D, KV_RANK + ROPE), D ** -0.5),
        'g_kv': draw_gain(6, KV_RANK),
        'w_ukv': draw_normal(7, (KV_RANK, HEADS * (NOPE + VDIM)), 1.5 * KV_RANK ** -0.5),
        'w_o': draw_normal(8, (HEADS * VDIM, D), (HEADS * VDIM) ** -0.5),
        'g_ffn': draw_gain(9, D),
        'w_gate': draw_normal(10, (EXPERTS, D, FF), D ** -0.5),
        'w_up': draw_normal(11, (EXPERTS, D, FF), D ** -0.5),
        'w_down': draw_normal(12, (EXPERTS, FF, D), 2.0 * FF ** -0.5),
        'ws_gate': draw_normal(13, (D, SHARED * FF), D ** -0.5),
        'ws_up': draw_normal(14, (D, SHARED * FF), D ** -0.5),
        'ws_down': draw_normal(15, (SHARED * FF, D), (SHARED * FF) ** -0.5),
    }


def reference(x_in, topk_idx, top_gate, g_attn, w_q, w_dkv, g_kv, w_ukv, w_o, g_ffn, w_gate, w_up, w_down, ws_gate, ws_up, ws_down):
    cos_tab, sin_tab = rope_tables(jnp.arange(SEQ), ROPE)
    causal = jnp.arange(SEQ)[:, None] >= jnp.arange(SEQ)[None, :]
    scale = (NOPE + ROPE) ** -0.5

    def attend_request(x_row):
        normed = rms_norm(x_row, g_attn)
        query = jnp.dot(normed, w_q, preferred_element_type=jnp.float32).astype(jnp.bfloat16).reshape(SEQ, HEADS, NOPE + ROPE)
        latent = jnp.dot(normed, w_dkv, preferred_element_type=jnp.float32)
        c_kv = rms_norm(latent[:, :KV_RANK], g_kv)
        k_rope = rotate(latent[:, KV_RANK:], cos_tab, sin_tab)
        key_val = jnp.dot(c_kv, w_ukv, preferred_element_type=jnp.float32).astype(jnp.bfloat16).reshape(SEQ, HEADS, NOPE + VDIM)
        q_rope = rotate(query[:, :, NOPE:], cos_tab[:, None, :], sin_tab[:, None, :])

        def one_head(head_args):
            q_nope_h, q_rope_h, k_nope_h, value_h = head_args
            scores = jnp.dot(q_nope_h, k_nope_h.T, preferred_element_type=jnp.float32) + jnp.dot(q_rope_h, k_rope.T, preferred_element_type=jnp.float32)
            scores = jnp.where(causal, scores * scale, -jnp.inf)
            attn_prob = jax.nn.softmax(scores, axis=-1).astype(jnp.bfloat16)
            return jnp.dot(attn_prob, value_h, preferred_element_type=jnp.float32).astype(jnp.bfloat16)

        heads_out = lax.map(one_head, (query[:, :, :NOPE].transpose(1, 0, 2), q_rope.transpose(1, 0, 2), key_val[:, :, :NOPE].transpose(1, 0, 2), key_val[:, :, NOPE:].transpose(1, 0, 2)))
        merged = heads_out.transpose(1, 0, 2).reshape(SEQ, HEADS * VDIM)
        attn = jnp.dot(merged, w_o, preferred_element_type=jnp.float32).astype(jnp.bfloat16)
        return attn, jnp.concatenate([c_kv, k_rope], axis=-1)

    attn_all, kv_cache = lax.map(attend_request, x_in)
    hidden = (x_in.astype(jnp.float32) + attn_all.astype(jnp.float32)).astype(jnp.bfloat16)
    tok_total = BATCH * SEQ
    normed = rms_norm(hidden, g_ffn).reshape(tok_total, D)
    flat_ids = topk_idx.reshape(tok_total * TOP)
    flat_gate = top_gate.reshape(tok_total * TOP)
    onehot = (flat_ids[:, None] == jnp.arange(EXPERTS)[None, :]).astype(jnp.int32)
    slot_rank = jnp.sum(jnp.cumsum(onehot, axis=0) * onehot, axis=1) - 1
    cap_all = CAP_DEV * TP * EP
    slot_ids = flat_ids * cap_all + slot_rank
    token_of_slot = jnp.full((EXPERTS * cap_all,), tok_total, jnp.int32).at[slot_ids].set(jnp.arange(tok_total * TOP, dtype=jnp.int32) // TOP).reshape(EXPERTS, cap_all)
    gate_of_slot = jnp.zeros((EXPERTS * cap_all,), jnp.float32).at[slot_ids].set(flat_gate).reshape(EXPERTS, cap_all)
    padded = jnp.concatenate([normed, jnp.zeros((1, D), jnp.bfloat16)], axis=0)

    def expert_step(running, expert_args):
        rows, weights, gate_mat, up_mat, down_mat = expert_args
        picked = padded[rows]
        act_gate = jnp.dot(picked, gate_mat, preferred_element_type=jnp.float32)
        act_up = jnp.dot(picked, up_mat, preferred_element_type=jnp.float32)
        act_hidden = (jax.nn.silu(act_gate) * act_up).astype(jnp.bfloat16)
        expert_out = jnp.dot(act_hidden, down_mat, preferred_element_type=jnp.float32).astype(jnp.bfloat16)
        return running.at[rows].add(weights[:, None] * expert_out.astype(jnp.float32)), None

    scan_out = lax.scan(expert_step, jnp.zeros((tok_total + 1, D), jnp.float32), (token_of_slot, gate_of_slot, w_gate, w_up, w_down))
    routed = scan_out[0][:tok_total]
    shared_gate = jnp.dot(normed, ws_gate, preferred_element_type=jnp.float32)
    shared_up = jnp.dot(normed, ws_up, preferred_element_type=jnp.float32)
    shared_act = (jax.nn.silu(shared_gate) * shared_up).astype(jnp.bfloat16)
    shared_out = jnp.dot(shared_act, ws_down, preferred_element_type=jnp.float32)
    y_sum = hidden.reshape(tok_total, D).astype(jnp.float32) + routed + shared_out
    y_out = y_sum.astype(jnp.bfloat16).reshape(BATCH, SEQ, D)
    return y_out, kv_cache
```

```python
import jax
import jax.numpy as jnp
from jax import lax
from jax.sharding import PartitionSpec as P

AXES = ('tp', 'ep')


def rms_norm(values, gain_vec):
    values32 = values.astype(jnp.float32)
    inv_rms = lax.rsqrt(jnp.mean(values32 * values32, axis=-1, keepdims=True) + 1e-6)
    return (values32 * inv_rms * gain_vec.astype(jnp.float32)).astype(jnp.bfloat16)


def rope_tables(positions, rope_dim):
    half_dim = rope_dim // 2
    inv_freq = 10000.0 ** (-2.0 * jnp.arange(half_dim, dtype=jnp.float32) / rope_dim)
    angles = positions.astype(jnp.float32)[:, None] * inv_freq[None, :]
    return jnp.cos(angles), jnp.sin(angles)


def rotate(values, cos_tab, sin_tab):
    half_dim = values.shape[-1] // 2
    first = values[..., :half_dim].astype(jnp.float32)
    second = values[..., half_dim:].astype(jnp.float32)
    return jnp.concatenate([first * cos_tab - second * sin_tab, second * cos_tab + first * sin_tab], axis=-1).astype(jnp.bfloat16)


def model_dims(w_q, w_dkv, g_kv, w_ukv, w_o):
    kv_rank = g_kv.shape[0]
    rope_dim = w_dkv.shape[1] - kv_rank
    heads = (w_q.shape[1] - w_ukv.shape[1] + w_o.shape[0]) // rope_dim
    return kv_rank, rope_dim, heads, w_q.shape[1] // heads - rope_dim, w_o.shape[0] // heads


def gather_weight(w_loc, ep_size):
    rows = w_loc.shape[0] // ep_size
    piece = lax.dynamic_slice_in_dim(w_loc, lax.axis_index('ep') * rows, rows, axis=0)
    return lax.all_gather(piece, AXES, axis=0, tiled=True)


def attend(query, key_val, k_rope, q_cos, q_sin, causal, nope_dim):
    rope_dim = k_rope.shape[-1]
    q_rope = rotate(query[..., nope_dim:], q_cos[:, None, :], q_sin[:, None, :])
    scores = jnp.einsum('bqhd,bkhd->bhqk', query[..., :nope_dim], key_val[..., :nope_dim], preferred_element_type=jnp.float32)
    scores = scores + jnp.einsum('crie,cle->cirl', q_rope, k_rope, preferred_element_type=jnp.float32)
    scores = jnp.where(causal, scores * (nope_dim + rope_dim) ** -0.5, -jnp.inf)
    attn_prob = jax.nn.softmax(scores, axis=-1).astype(jnp.bfloat16)
    return jnp.einsum('bhqk,bkhd->bqhd', attn_prob, key_val[..., nope_dim:], preferred_element_type=jnp.float32).astype(jnp.bfloat16)


def routing_tables(ids_loc, expert_count, dev_count, capacity):
    tok_dev, top_k = ids_loc.shape
    local_experts = expert_count // dev_count
    flat_ids = ids_loc.reshape(tok_dev * top_k)
    onehot = (flat_ids[:, None] == jnp.arange(expert_count)[None, :]).astype(jnp.int32)
    running = jnp.cumsum(onehot, axis=0)
    slot_rank = jnp.sum(running * onehot, axis=1) - 1
    slot_ids = flat_ids * capacity + slot_rank
    token_of_slot = jnp.zeros((expert_count * capacity,), jnp.int32).at[slot_ids].set(jnp.arange(tok_dev * top_k, dtype=jnp.int32) // top_k, mode='promise_in_bounds', unique_indices=True)
    tokens = lax.all_to_all(token_of_slot.reshape(dev_count, local_experts * capacity), AXES, 0, 0, tiled=True)
    tokens = tokens.reshape(dev_count, local_experts, capacity)
    load = lax.pmax(running[-1], AXES).reshape(dev_count, local_experts)
    index = jnp.arange(local_experts)
    ahead = (load[:, None, :] > load[:, :, None]) | ((load[:, None, :] == load[:, :, None]) & (index[None, None, :] < index[None, :, None]))
    position = jnp.sum(ahead.astype(jnp.int32), axis=2)
    chosen = (position[:, None, :] == index[None, :, None]).astype(jnp.int32)
    order = jnp.sum(chosen * index[None, None, :], axis=2)
    peak = jnp.max(jnp.sum(chosen * load[:, None, :], axis=2), axis=0)
    slot_position = jnp.sum(onehot * position.reshape(1, expert_count), axis=1)
    return tokens, order, peak, flat_ids // local_experts, slot_position, slot_rank


def expert_pass(caps, pieces, operands):
    normed_all, tokens, order, slot_device, slot_position, slot_rank, gate_loc, hidden, shared_out, w_gate, w_up, w_down = operands
    dev_count = tokens.shape[0]
    tok_dev, width = hidden.shape
    top_k = gate_loc.shape[-1]
    first_row = (jnp.arange(dev_count, dtype=jnp.int32) * tok_dev)[:, None]
    total = dev_count * sum(caps)
    returned = jnp.zeros((total, width), jnp.bfloat16)
    slot_row = jnp.zeros_like(slot_rank)
    base = 0
    for place, cap in enumerate(caps):
        expert = order[place]
        gate_mat = lax.dynamic_index_in_dim(w_gate, expert, 0, keepdims=False)
        up_mat = lax.dynamic_index_in_dim(w_up, expert, 0, keepdims=False)
        down_mat = lax.dynamic_index_in_dim(w_down, expert, 0, keepdims=False)
        mine = lax.dynamic_index_in_dim(tokens, expert, 1, keepdims=False)
        step = cap // pieces[place]
        rank = jnp.minimum(slot_rank, cap - 1)
        slot_row = jnp.where(slot_position == place, base + (rank // step) * (dev_count * step) + slot_device * step + rank % step, slot_row)
        for piece in range(pieces[place]):
            rows = (mine[:, piece * step:(piece + 1) * step] + first_row).reshape(dev_count * step)
            picked = normed_all.at[rows].get(mode='promise_in_bounds')
            act_gate = jnp.dot(picked, gate_mat, preferred_element_type=jnp.float32)
            act_up = jnp.dot(picked, up_mat, preferred_element_type=jnp.float32)
            act_hidden = (jax.nn.silu(act_gate) * act_up).astype(jnp.bfloat16)
            expert_out = jnp.dot(act_hidden, down_mat, preferred_element_type=jnp.float32).astype(jnp.bfloat16)
            arrived = lax.all_to_all(expert_out.reshape(dev_count, step, width), AXES, 0, 0, tiled=True)
            returned = lax.dynamic_update_slice(returned, arrived.reshape(dev_count * step, width), (base, 0))
            base += dev_count * step
    back = returned.at[slot_row.reshape(tok_dev, top_k).T.reshape(top_k * tok_dev)].get(mode='promise_in_bounds', unique_indices=True)
    gates = gate_loc.T
    routed = jnp.sum(gates[:, :, None] * back.reshape(top_k, tok_dev, width).astype(jnp.float32), axis=0)
    return (hidden.astype(jnp.float32) + routed + shared_out).astype(jnp.bfloat16)


def moe_block(hidden, tables, gate_loc, g_ffn, w_gate, w_up, w_down, ws_gate, ws_up, ws_down, capacity):
    bat_loc, seq_loc, width = hidden.shape
    tok_dev = bat_loc * seq_loc
    tokens, order, peak, slot_device, slot_position, slot_rank = tables
    dev_count, local_experts = tokens.shape[:2]
    normed = rms_norm(hidden, g_ffn).reshape(tok_dev, width)
    normed_all = lax.all_gather(normed, AXES, axis=0, tiled=True)
    shared_gate = jnp.dot(normed, ws_gate, preferred_element_type=jnp.float32)
    shared_up = jnp.dot(normed, ws_up, preferred_element_type=jnp.float32)
    shared_act = (jax.nn.silu(shared_gate) * shared_up).astype(jnp.bfloat16)
    shared_out = jnp.dot(shared_act, ws_down, preferred_element_type=jnp.float32)
    device = lax.axis_index('tp') * (dev_count // lax.axis_size('tp')) + lax.axis_index('ep')
    own_order = lax.dynamic_index_in_dim(order, device, 0, keepdims=False)
    small = capacity // 6
    branches = []
    for full in range(2, local_experts + 1):
        caps = [capacity] * full + [small] * (local_experts - full)
        pieces = [2] * full + [1] * (local_experts - full)
        branches.append(lambda *ops, caps=caps, pieces=pieces: expert_pass(caps, pieces, ops))
    heavy = jnp.sum((peak > small).astype(jnp.int32))
    choice = jnp.clip(heavy - 2, 0, len(branches) - 1)
    y_sum = lax.switch(choice, branches, normed_all, tokens, own_order, slot_device, slot_position, slot_rank, gate_loc.reshape(tok_dev, -1), hidden.reshape(tok_dev, width), shared_out, w_gate, w_up, w_down)
    return y_sum.reshape(bat_loc, seq_loc, width)


def solution(mesh):
    tp_size = mesh.shape['tp']
    ep_size = mesh.shape['ep']
    dev_count = tp_size * ep_size
    token_spec = P('ep', 'tp', None)
    expert_spec = P(('tp', 'ep'), None, None)
    in_specs = (token_spec, token_spec, token_spec, P(None), P(None, 'tp'), P(None, None), P(None), P(None, 'tp'), P('tp', None), P(None), expert_spec, expert_spec, expert_spec, P(None, None), P(None, None), P(None, None))

    def layer(x_in, topk_idx, top_gate, g_attn, w_q, w_dkv, g_kv, w_ukv, w_o, g_ffn, w_gate, w_up, w_down, ws_gate, ws_up, ws_down):
        kv_rank, rope_dim, heads, nope_dim, value_dim = model_dims(w_q, w_dkv, g_kv, w_ukv, w_o)
        expert_count = w_gate.shape[0]

        def device_layer(x_loc, ids_loc, gate_loc, g_attn, w_q, w_dkv, g_kv, w_ukv, w_o, g_ffn, w_gate, w_up, w_down, ws_gate, ws_up, ws_down):
            bat_loc, seq_loc, width = x_loc.shape
            seq_len = seq_loc * tp_size
            heads_loc = w_o.shape[0] // value_dim
            tp_index = lax.axis_index('tp')
            tok_dev, top_k = bat_loc * seq_loc, ids_loc.shape[-1]
            capacity = 3 * (tok_dev * top_k // expert_count)
            tables = routing_tables(ids_loc.reshape(tok_dev, top_k), expert_count, dev_count, capacity)
            w_q_all = gather_weight(w_q, ep_size).reshape(tp_size, width, w_q.shape[1])
            w_ukv_all = gather_weight(w_ukv, ep_size).reshape(tp_size, kv_rank, w_ukv.shape[1])
            w_o_all = gather_weight(w_o, ep_size)
            normed = rms_norm(x_loc, g_attn)
            latent = jnp.einsum('bsd,dn->bsn', normed, w_dkv, preferred_element_type=jnp.float32)
            positions = tp_index * seq_loc + jnp.arange(seq_loc)
            cos_tab, sin_tab = rope_tables(positions, rope_dim)
            c_kv = rms_norm(latent[..., :kv_rank], g_kv)
            k_rope = rotate(latent[..., kv_rank:], cos_tab, sin_tab)
            cache_loc = jnp.concatenate([c_kv, k_rope], axis=-1)
            cache_full = lax.all_gather(cache_loc, 'tp', axis=1, tiled=True)
            causal = positions[:, None] >= jnp.arange(seq_len)[None, :]
            heads_out = []
            for part in range(tp_size):
                query = jnp.einsum('bsd,dn->bsn', normed, w_q_all[part], preferred_element_type=jnp.float32).astype(jnp.bfloat16).reshape(bat_loc, seq_loc, heads_loc, nope_dim + rope_dim)
                key_val = jnp.einsum('bsr,rn->bsn', cache_full[..., :kv_rank], w_ukv_all[part], preferred_element_type=jnp.float32).astype(jnp.bfloat16).reshape(bat_loc, seq_len, heads_loc, nope_dim + value_dim)
                part_out = attend(query, key_val, cache_full[..., kv_rank:], cos_tab, sin_tab, causal, nope_dim)
                heads_out.append(part_out.reshape(bat_loc, seq_loc, heads_loc * value_dim))
            merged = jnp.concatenate(heads_out, axis=-1)
            attn = jnp.einsum('bsn,nd->bsd', merged, w_o_all, preferred_element_type=jnp.float32).astype(jnp.bfloat16)
            hidden = (x_loc.astype(jnp.float32) + attn.astype(jnp.float32)).astype(jnp.bfloat16)
            y_loc = moe_block(hidden, tables, gate_loc, g_ffn, w_gate, w_up, w_down, ws_gate, ws_up, ws_down, capacity)
            return y_loc, cache_loc

        return jax.shard_map(device_layer, mesh=mesh, in_specs=in_specs, out_specs=(token_spec, token_spec), check_vma=False)(x_in, topk_idx, top_gate, g_attn, w_q, w_dkv, g_kv, w_ukv, w_o, g_ffn, w_gate, w_up, w_down, ws_gate, ws_up, ws_down)

    return layer
```

```python
import functools

import jax
import jax.numpy as jnp
from jax import lax
from jax.experimental import pallas as pl
from jax.experimental.pallas import tpu as pltpu
from jax.sharding import PartitionSpec as P

AXES = ('tp', 'ep')


def rms_norm(values, gain_vec):
    values32 = values.astype(jnp.float32)
    inv_rms = lax.rsqrt(jnp.mean(values32 * values32, axis=-1, keepdims=True) + 1e-6)
    return (values32 * inv_rms * gain_vec.astype(jnp.float32)).astype(jnp.bfloat16)


def rope_tables(positions, rope_dim):
    half_dim = rope_dim // 2
    inv_freq = 10000.0 ** (-2.0 * jnp.arange(half_dim, dtype=jnp.float32) / rope_dim)
    angles = positions.astype(jnp.float32)[:, None] * inv_freq[None, :]
    return jnp.cos(angles), jnp.sin(angles)


def rotate(values, cos_tab, sin_tab):
    half_dim = values.shape[-1] // 2
    first = values[..., :half_dim].astype(jnp.float32)
    second = values[..., half_dim:].astype(jnp.float32)
    return jnp.concatenate([first * cos_tab - second * sin_tab, second * cos_tab + first * sin_tab], axis=-1).astype(jnp.bfloat16)


def model_dims(w_q, w_dkv, g_kv, w_ukv, w_o):
    kv_rank = g_kv.shape[0]
    rope_dim = w_dkv.shape[1] - kv_rank
    heads = (w_q.shape[1] - w_ukv.shape[1] + w_o.shape[0]) // rope_dim
    return kv_rank, rope_dim, heads, w_q.shape[1] // heads - rope_dim, w_o.shape[0] // heads


def gather_weight(w_loc, ep_size):
    rows = w_loc.shape[0] // ep_size
    piece = lax.dynamic_slice_in_dim(w_loc, lax.axis_index('ep') * rows, rows, axis=0)
    return lax.all_gather(piece, AXES, axis=0, tiled=True)


def attend(query, key_val, k_rope, q_cos, q_sin, causal, nope_dim):
    rope_dim = k_rope.shape[-1]
    q_rope = rotate(query[..., nope_dim:], q_cos[:, None, :], q_sin[:, None, :])
    scores = jnp.einsum('bqhd,bkhd->bhqk', query[..., :nope_dim], key_val[..., :nope_dim], preferred_element_type=jnp.float32)
    scores = scores + jnp.einsum('crie,cle->cirl', q_rope, k_rope, preferred_element_type=jnp.float32)
    scores = jnp.where(causal, scores * (nope_dim + rope_dim) ** -0.5, -jnp.inf)
    attn_prob = jax.nn.softmax(scores, axis=-1).astype(jnp.bfloat16)
    return jnp.einsum('bhqk,bkhd->bqhd', attn_prob, key_val[..., nope_dim:], preferred_element_type=jnp.float32).astype(jnp.bfloat16)


def routing_tables(ids_loc, gate_loc, later, expert_count, dev_count, capacity):
    tok_dev, top_k = ids_loc.shape
    local_experts = expert_count // dev_count
    flat_ids = ids_loc.reshape(tok_dev * top_k)
    onehot = (flat_ids[:, None] == jnp.arange(expert_count)[None, :]).astype(jnp.int32)
    running = jnp.cumsum(onehot, axis=0)
    slot_rank = jnp.sum(running * onehot, axis=1) - 1
    slot_ids = flat_ids * capacity + slot_rank
    slots = expert_count * capacity
    token_of_slot = jnp.full((slots,), -1, jnp.int32).at[slot_ids].set(jnp.arange(tok_dev * top_k, dtype=jnp.int32) // top_k, mode='promise_in_bounds', unique_indices=True)
    gate_of_slot = jnp.zeros((slots,), jnp.float32).at[slot_ids].set(gate_loc.reshape(tok_dev * top_k), mode='promise_in_bounds', unique_indices=True)
    gate_of_slot, later = lax.optimization_barrier((gate_of_slot, later))
    tokens = lax.all_to_all(token_of_slot.reshape(dev_count, local_experts * capacity), AXES, 0, 0, tiled=True)
    tokens = tokens.reshape(dev_count, local_experts, capacity)
    load = lax.pmax(running[-1], AXES).reshape(dev_count, local_experts)
    index = jnp.arange(local_experts)
    ahead = (load[:, None, :] > load[:, :, None]) | ((load[:, None, :] == load[:, :, None]) & (index[None, None, :] < index[None, :, None]))
    position = jnp.sum(ahead.astype(jnp.int32), axis=2)
    chosen = (position[:, None, :] == index[None, :, None]).astype(jnp.int32)
    order = jnp.sum(chosen * index[None, None, :], axis=2)
    peak = jnp.max(jnp.sum(chosen * load[:, None, :], axis=2), axis=0)
    own_tokens = place_rows(chosen, token_of_slot.reshape(dev_count, local_experts, capacity))
    own_gates = place_rows(chosen, gate_of_slot.reshape(dev_count, local_experts, capacity))
    own_counts = place_rows(chosen, running[-1].reshape(dev_count, local_experts, 1))[..., 0]
    own_tokens = jnp.where(own_tokens < 0, tok_dev, own_tokens)
    return (tokens, order, peak, own_tokens, own_gates, own_counts), later


def place_rows(chosen, by_expert):
    picked = jnp.where(chosen[..., None] > 0, by_expert[:, None], jnp.zeros((), by_expert.dtype))
    return jnp.sum(picked, axis=2)


def pick_kernel(steps, tile, parts, low_ref, high_ref, tok_ref, *rest):
    tables, outs, total_ref = rest[:parts], rest[parts:-1], rest[-1]
    tiles = tables[0].shape[1] // tile
    source = pl.program_id(0)
    start = 0
    for piece, step in enumerate(steps):
        wanted = tok_ref[0, start:start + step, :]
        total_ref[:step, :] = jnp.zeros((step, total_ref.shape[1]), jnp.float32)

        where = source * len(steps) + piece
        for part, table_ref in enumerate(tables):

            def add_tile(index, carry, wanted=wanted, step=step, part=part, table_ref=table_ref):
                seen = lax.broadcasted_iota(jnp.int32, (step, tile), 1) + index * tile
                onehot = jnp.where(wanted == seen, 1.0, 0.0).astype(jnp.bfloat16)
                first = pl.multiple_of((index - part * tiles) * tile, tile)
                total_ref[:step, :] += jnp.dot(onehot, table_ref[0, pl.ds(first, tile), :], preferred_element_type=jnp.float32)
                return carry

            lax.fori_loop(jnp.maximum(low_ref[where], part * tiles), jnp.minimum(high_ref[where], (part + 1) * tiles), add_tile, 0)
        outs[piece][0] = total_ref[:step, :].astype(jnp.bfloat16)
        start += step


def pick_rows(tables, wanted, steps):
    dev_count, tok_part, width = tables[0].shape
    tok_dev = tok_part * len(tables)
    tile = 256 if tok_part % 256 == 0 else tok_part
    lows, highs, start = [], [], 0
    for step in steps:
        part = wanted[:, start:start + step]
        lows.append(jnp.min(jnp.where(part < 0, tok_dev, part), axis=1) // tile)
        highs.append((jnp.max(part, axis=1) + tile) // tile)
        start += step
    low, high = jnp.stack(lows, axis=1).reshape(-1), jnp.stack(highs, axis=1).reshape(-1)
    grid_spec = pltpu.PrefetchScalarGridSpec(
        num_scalar_prefetch=2,
        grid=(dev_count,),
        in_specs=[pl.BlockSpec((1, start, 1), lambda i, *_: (i, 0, 0)), *[pl.BlockSpec((1, tok_part, width), lambda i, *_: (i, 0, 0)) for _ in tables]],
        out_specs=[pl.BlockSpec((1, step, width), lambda i, *_: (i, 0, 0)) for step in steps],
        scratch_shapes=[pltpu.VMEM((max(steps), width), jnp.float32)],
    )
    rows = dev_count * start
    return pl.pallas_call(
        functools.partial(pick_kernel, steps, tile, len(tables)),
        grid_spec=grid_spec,
        out_shape=[jax.ShapeDtypeStruct((dev_count, step, width), jnp.bfloat16) for step in steps],
        compiler_params=pltpu.CompilerParams(dimension_semantics=('arbitrary',), vmem_limit_bytes=40 * 1024 * 1024),
        cost_estimate=pl.CostEstimate(flops=rows * tok_dev * width, bytes_accessed=2 * (dev_count * tok_dev + rows) * width, transcendentals=0),
        name='pick_rows',
    )(low, high, wanted[:, :start, None], *tables)


def combine_kernel(step, count_ref, tok_ref, gate_ref, rows_ref, before_ref, after_ref, sums, rows32, sem):
    source = pl.program_id(0)
    tok_dev = before_ref.shape[0]

    @pl.when(source == 0)
    def _():
        load = pltpu.make_async_copy(before_ref, sums.at[pl.ds(0, tok_dev)], sem)
        load.start()
        load.wait()

    rows32[...] = rows_ref[0].astype(jnp.float32)
    base = source * step

    def add_rows(index, carry):
        first = index * 4
        where = [tok_ref[base + first + j] for j in range(4)]
        added = [sums[pl.ds(where[j], 1), :] + gate_ref[base + first + j] * rows32[pl.ds(first + j, 1), :] for j in range(4)]
        for j in range(4):
            sums[pl.ds(where[j], 1), :] = added[j]
        return carry

    lax.fori_loop(0, (count_ref[source] + 3) // 4, add_rows, 0)

    @pl.when(source == pl.num_programs(0) - 1)
    def _():
        store = pltpu.make_async_copy(sums.at[pl.ds(0, tok_dev)], after_ref, sem)
        store.start()
        store.wait()


def combine(sums, rows, counts, tokens, gates):
    dev_count, step, width = rows.shape
    tok_dev = sums.shape[0]
    grid_spec = pltpu.PrefetchScalarGridSpec(
        num_scalar_prefetch=3,
        grid=(dev_count,),
        in_specs=[pl.BlockSpec((1, step, width), lambda i, *_: (i, 0, 0)), pl.BlockSpec(memory_space=pl.ANY)],
        out_specs=pl.BlockSpec(memory_space=pl.ANY),
        scratch_shapes=[pltpu.VMEM((tok_dev + 8, width), jnp.float32), pltpu.VMEM((step, width), jnp.float32), pltpu.SemaphoreType.DMA],
    )
    return pl.pallas_call(
        functools.partial(combine_kernel, step),
        grid_spec=grid_spec,
        out_shape=jax.ShapeDtypeStruct(sums.shape, sums.dtype),
        input_output_aliases={4: 0},
        compiler_params=pltpu.CompilerParams(dimension_semantics=('arbitrary',), vmem_limit_bytes=32 * 1024 * 1024),
        cost_estimate=pl.CostEstimate(flops=dev_count * step * width * 400, bytes_accessed=2 * rows.size + 8 * sums.size, transcendentals=0),
        name='combine',
    )(counts, tokens.reshape(-1), gates.reshape(-1), rows, sums)


def expert_pass(plan, operands):
    tables, tokens, order, own_tokens, own_gates, own_counts, sums, w_gate, w_up, w_down = operands
    dev_count = tokens.shape[0]
    width = sums.shape[1]
    tables = [table.reshape(dev_count, -1, width) for table in tables]
    for place, steps in plan:
        expert = order[place]
        gate_mat = lax.dynamic_index_in_dim(w_gate, expert, 0, keepdims=False)
        up_mat = lax.dynamic_index_in_dim(w_up, expert, 0, keepdims=False)
        down_mat = lax.dynamic_index_in_dim(w_down, expert, 0, keepdims=False)
        mine = lax.dynamic_index_in_dim(tokens, expert, 1, keepdims=False)
        start = 0
        for step, picked in zip(steps, pick_rows(tables, mine, steps)):
            picked = picked.reshape(dev_count * step, width)
            act_gate = jnp.dot(picked, gate_mat, preferred_element_type=jnp.float32)
            act_up = jnp.dot(picked, up_mat, preferred_element_type=jnp.float32)
            act_hidden = (jax.nn.silu(act_gate) * act_up).astype(jnp.bfloat16)
            expert_out = jnp.dot(act_hidden, down_mat, preferred_element_type=jnp.float32).astype(jnp.bfloat16)
            arrived = lax.all_to_all(expert_out.reshape(dev_count, step, width), AXES, 0, 0, tiled=True)
            used = jnp.clip(own_counts[:, place] - start, 0, step)
            sums = combine(sums, arrived, used, own_tokens[:, place, start:start + step], own_gates[:, place, start:start + step])
            start += step
    return sums.astype(jnp.bfloat16)


def send_tokens(hidden, earlier, g_ffn, ws_gate, ws_up, ws_down):
    width = hidden.shape[-1]
    hidden = hidden.reshape(-1, width)
    normed = rms_norm(hidden, g_ffn)
    if earlier:
        normed, earlier[-1] = lax.optimization_barrier((normed, earlier[-1]))
    earlier.append(lax.all_gather(normed, AXES, axis=0, tiled=True))
    shared_gate = jnp.dot(normed, ws_gate, preferred_element_type=jnp.float32)
    shared_up = jnp.dot(normed, ws_up, preferred_element_type=jnp.float32)
    shared_act = (jax.nn.silu(shared_gate) * shared_up).astype(jnp.bfloat16)
    shared_out = jnp.dot(shared_act, ws_down, preferred_element_type=jnp.float32)
    return normed, hidden.astype(jnp.float32) + shared_out


def route(normed_parts, sums, tables, w_gate, w_up, w_down, capacity):
    tokens, order, peak, own_tokens, own_gates, own_counts = tables
    dev_count, local_experts = tokens.shape[:2]
    device = lax.axis_index('tp') * (dev_count // lax.axis_size('tp')) + lax.axis_index('ep')
    own_order = lax.dynamic_index_in_dim(order, device, 0, keepdims=False)
    small = -(-capacity // 96) * 16
    first = -(-capacity // 32) * 16
    branches = []
    for full in range(2, local_experts + 1):
        big = [(place, (first, capacity - first)) for place in range(full)]
        light = [(place, (small,)) for place in range(full, local_experts)]
        plan = light[-1:] + big + light[:-1]
        branches.append(lambda *ops, plan=plan: expert_pass(plan, ops))
    heavy = jnp.sum((peak > small).astype(jnp.int32))
    choice = jnp.clip(heavy - 2, 0, len(branches) - 1)
    return lax.switch(choice, branches, normed_parts, tokens, own_order, own_tokens, own_gates, own_counts, sums, w_gate, w_up, w_down)


def solution(mesh):
    tp_size = mesh.shape['tp']
    ep_size = mesh.shape['ep']
    dev_count = tp_size * ep_size
    token_spec = P('ep', 'tp', None)
    expert_spec = P(('tp', 'ep'), None, None)
    in_specs = (token_spec, token_spec, token_spec, P(None), P(None, 'tp'), P(None, None), P(None), P(None, 'tp'), P('tp', None), P(None), expert_spec, expert_spec, expert_spec, P(None, None), P(None, None), P(None, None))

    def layer(x_in, topk_idx, top_gate, g_attn, w_q, w_dkv, g_kv, w_ukv, w_o, g_ffn, w_gate, w_up, w_down, ws_gate, ws_up, ws_down):
        kv_rank, rope_dim, heads, nope_dim, value_dim = model_dims(w_q, w_dkv, g_kv, w_ukv, w_o)
        expert_count = w_gate.shape[0]

        def device_layer(x_loc, ids_loc, gate_loc, g_attn, w_q, w_dkv, g_kv, w_ukv, w_o, g_ffn, w_gate, w_up, w_down, ws_gate, ws_up, ws_down):
            bat_loc, seq_loc, width = x_loc.shape
            seq_len = seq_loc * tp_size
            heads_loc = w_o.shape[0] // value_dim
            tp_index = lax.axis_index('tp')
            tok_dev, top_k = bat_loc * seq_loc, ids_loc.shape[-1]
            capacity = 3 * (tok_dev * top_k // expert_count)
            w_q_all = gather_weight(w_q, ep_size).reshape(tp_size, width, w_q.shape[1])
            w_ukv_all = gather_weight(w_ukv, ep_size).reshape(tp_size, kv_rank, w_ukv.shape[1])
            w_o_all = gather_weight(w_o, ep_size)
            normed = rms_norm(x_loc, g_attn)
            tables, queries_in = routing_tables(ids_loc.reshape(tok_dev, top_k), gate_loc, normed, expert_count, dev_count, capacity)
            latent = jnp.einsum('bsd,dn->bsn', normed, w_dkv, preferred_element_type=jnp.float32)
            positions = tp_index * seq_loc + jnp.arange(seq_loc)
            cos_tab, sin_tab = rope_tables(positions, rope_dim)
            c_kv = rms_norm(latent[..., :kv_rank], g_kv)
            k_rope = rotate(latent[..., kv_rank:], cos_tab, sin_tab)
            cache_loc = jnp.concatenate([c_kv, k_rope], axis=-1)
            cache_full = lax.all_gather(cache_loc, 'tp', axis=1, tiled=True)
            causal = positions[:, None] >= jnp.arange(seq_len)[None, :]
            groups = 2 if bat_loc % 2 == 0 else 1
            group = bat_loc // groups
            normed_parts, sums_parts, sent = [], [], None
            for index in range(groups):
                mine = slice(index * group, (index + 1) * group)
                cache, tokens_in = cache_full[mine], queries_in[mine]
                if sent is not None:
                    tokens_in, _ = lax.optimization_barrier((tokens_in, sent))
                heads_out = []
                for part in range(tp_size):
                    query = jnp.einsum('bsd,dn->bsn', tokens_in, w_q_all[part], preferred_element_type=jnp.float32).astype(jnp.bfloat16).reshape(group, seq_loc, heads_loc, nope_dim + rope_dim)
                    key_val = jnp.einsum('bsr,rn->bsn', cache[..., :kv_rank], w_ukv_all[part], preferred_element_type=jnp.float32).astype(jnp.bfloat16).reshape(group, seq_len, heads_loc, nope_dim + value_dim)
                    part_out = attend(query, key_val, cache[..., kv_rank:], cos_tab, sin_tab, causal, nope_dim)
                    heads_out.append(part_out.reshape(group, seq_loc, heads_loc * value_dim))
                merged = jnp.concatenate(heads_out, axis=-1)
                attn = jnp.einsum('bsn,nd->bsd', merged, w_o_all, preferred_element_type=jnp.float32).astype(jnp.bfloat16)
                hidden = (x_loc[mine].astype(jnp.float32) + attn.astype(jnp.float32)).astype(jnp.bfloat16)
                sent, sums = send_tokens(hidden, normed_parts, g_ffn, ws_gate, ws_up, ws_down)
                sums_parts.append(sums)
            y_loc = route(normed_parts, jnp.concatenate(sums_parts, axis=0), tables, w_gate, w_up, w_down, capacity).reshape(bat_loc, seq_loc, width)
            return y_loc, cache_loc

        return jax.shard_map(device_layer, mesh=mesh, in_specs=in_specs, out_specs=(token_spec, token_spec), check_vma=False)(x_in, topk_idx, top_gate, g_attn, w_q, w_dkv, g_kv, w_ukv, w_o, g_ffn, w_gate, w_up, w_down, ws_gate, ws_up, ws_down)

    return layer
```
